32 devices in a mesh: fsdp: 8 (over z, x), model: 4 (over y, core).
Axes of the slice: x: 2, y: 2, z: 4, core: 2. Of those that a mesh axis runs over, the one named last changes fastest.
Arguments:
- weight_query: bfloat16 [5120, 8192], P('fsdp', 'model'), may hold values from -0.125 to 0.125
- low_query: bfloat16 [5120, 32], P('fsdp'), may hold values from -0.078125 to 0.078125
- high_query: bfloat16 [32, 8192], P(None, 'model'), may hold values from -1 to 1
- weight_key: bfloat16 [5120, 1024], P('fsdp', 'model'), may hold values from -0.125 to 0.125
- low_key: bfloat16 [5120, 32], P('fsdp'), may hold values from -0.078125 to 0.078125
- high_key: bfloat16 [32, 1024], P(None, 'model'), may hold values from -1 to 1
- weight_value: bfloat16 [5120, 1024], P('fsdp', 'model'), may hold values from -0.125 to 0.125
- low_value: bfloat16 [5120, 32], P('fsdp'), may hold values from -0.078125 to 0.078125
- high_value: bfloat16 [32, 1024], P(None, 'model'), may hold values from -1 to 1
- norm_train: float32 [5120], P(('fsdp', 'model')), may hold values from 0.25 to 1.75
- norm_step: float32 [5120], P(('fsdp', 'model')), may hold values from -0.3 to 0.3
Outputs:
- final_query: bfloat16 [5120, 8192], P(None, 'model')
- final_key: bfloat16 [5120, 1024], P(None, 'model')
- final_value: bfloat16 [5120, 1024], P(None, 'model')
- column_query: float32 [8192], P('model')
- column_key: float32 [1024], P('model')
- column_value: float32 [1024], P('model')
- serve_norm: bfloat16 [5120], replicated
The draws below stay inside these ranges and needn't reach their ends.
All inputs are finite; a program needn't handle non-finite values. Where the reference program divides by a largest or mean magnitude, that divisor is 1e-20 or more.
Results may differ from the reference program's by a relative error of at most 0.001.
Values may be sent and summed in bfloat16 or wider, within the bound.
A program may use at most 128 MiB of HBM per device.

```python
import jax
import jax.numpy as jnp

D_MODEL = 5120
Q_DIM = 8192
KV_DIM = 1024
RANK = 32


def strengthened(drawn, key, source, target, blocks, factor):
    owner, partner = [(jnp.arange(drawn.shape[dim]) // (drawn.shape[dim] // blocks)).reshape([-1 if axis == dim else 1 for axis in range(drawn.ndim)]) for dim in (source, target)]
    chosen = jax.random.permutation(key, blocks)[partner]
    strong = (owner == chosen) | (owner == (partner + blocks // 2) % blocks)
    return jnp.where(strong, factor * drawn, drawn)


def block_levels(key, dims, cuts, low, top_value):
    def one(axis_at, parts):
        draws = jax.random.uniform(jax.random.fold_in(jax.random.fold_in(key, 6), axis_at), (parts,), jnp.float32, low / len(cuts), top_value / len(cuts))
        return jnp.repeat(jnp.exp(draws), dims[axis_at] // parts).reshape((-1,) + (1,) * (len(dims) - axis_at - 1))

    loudness = one(*cuts[0])
    for cut in cuts[1:]:
        loudness = loudness * one(*cut)
    return loudness


def noise(own_key, dims, spread, reach, shards=(), dtype=jnp.bfloat16):
    array = spread * jax.random.normal(own_key, dims, jnp.float32)
    if shards:
        array = array * block_levels(own_key, dims, shards, -0.22, 0.18)
    return jnp.clip(array, -reach, reach).astype(dtype)


def bell_draw_with(own_key, dims, deviation, most, shards, heavy, kind=jnp.bfloat16):
    entries = deviation * jax.random.normal(own_key, dims, jnp.float32)
    if shards:
        entries = entries * block_levels(own_key, dims, shards, -0.22, 0.18)
    return jnp.clip(strengthened(entries, jax.random.fold_in(own_key, 3), *heavy), -most, most).astype(kind)


def setup_inputs(seed: int = 0) -> dict:
    seeds = jax.random.split(jax.random.key(seed), 12)
    weight_query = bell_draw_with(seeds[0], (D_MODEL, Q_DIM), D_MODEL ** -0.5, 0.125, ((0, 8), (1, 4)), (0, 1, 8, 2.0))
    low_query = noise(seeds[1], (D_MODEL, RANK), D_MODEL ** -0.5, 0.078125, ((0, 8),))
    high_query = noise(seeds[2], (RANK, Q_DIM), RANK ** -0.5, 1.0, ((1, 4),))
    weight_key = bell_draw_with(seeds[3], (D_MODEL, KV_DIM), D_MODEL ** -0.5, 0.125, ((0, 8), (1, 4)), (0, 1, 8, 2.0))
    low_key = noise(seeds[4], (D_MODEL, RANK), D_MODEL ** -0.5, 0.078125, ((0, 8),))
    high_key = noise(seeds[5], (RANK, KV_DIM), RANK ** -0.5, 1.0, ((1, 4),))
    weight_value = bell_draw_with(seeds[6], (D_MODEL, KV_DIM), D_MODEL ** -0.5, 0.125, ((0, 8), (1, 4)), (0, 1, 8, 2.0))
    low_value = noise(seeds[7], (D_MODEL, RANK), D_MODEL ** -0.5, 0.078125, ((0, 8),))
    high_value = noise(seeds[8], (RANK, KV_DIM), RANK ** -0.5, 1.0, ((1, 4),))
    norm_train = jnp.clip(1.0 + 0.15 * jax.random.normal(seeds[9], (D_MODEL,), jnp.float32), 0.25, 1.75)
    norm_step = jnp.clip(jax.random.uniform(seeds[10], (D_MODEL,), jnp.float32, -0.3, 0.3) * block_levels(seeds[10], (D_MODEL,), ((0, 32),), -0.4, 0.0), -0.3, 0.3)
    return dict(weight_query=weight_query, low_query=low_query, high_query=high_query, weight_key=weight_key, low_key=low_key, high_key=high_key, weight_value=weight_value, low_value=low_value, high_value=high_value, norm_train=norm_train, norm_step=norm_step)


mix_rate = 0.5


def reference(weight_query, low_query, high_query, weight_key, low_key, high_key, weight_value, low_value, high_value, norm_train, norm_step):
    result_query = weight_query.astype(jnp.float32) + mix_rate * jnp.dot(low_query, high_query, preferred_element_type=jnp.float32)
    result_key = weight_key.astype(jnp.float32) + mix_rate * jnp.dot(low_key, high_key, preferred_element_type=jnp.float32)
    result_value = weight_value.astype(jnp.float32) + mix_rate * jnp.dot(low_value, high_value, preferred_element_type=jnp.float32)
    column_query = jnp.max(jnp.abs(result_query), axis=0)
    final_query = (result_query / column_query).astype(jnp.bfloat16)
    column_key = jnp.max(jnp.abs(result_key), axis=0)
    final_key = (result_key / column_key).astype(jnp.bfloat16)
    column_value = jnp.max(jnp.abs(result_value), axis=0)
    final_value = (result_value / column_value).astype(jnp.bfloat16)
    serve_norm = (norm_train + norm_step).astype(jnp.bfloat16)
    return final_query, final_key, final_value, column_query, column_key, column_value, serve_norm
```

```python
import functools

import jax
import jax.numpy as jnp
from jax import lax
from jax.experimental import pallas as pl
from jax.experimental.pallas import tpu as pltpu
from jax.sharding import PartitionSpec as P

mix_rate = 0.5
MESH = pl.DeviceIdType.MESH
QUERY_PIECES = 4


def split_rows(rows, parts):
    tiles = rows // 16
    parts = min(parts, tiles)
    edges = [16 * (tiles * i // parts) for i in range(parts + 1)]
    return [(a, b - a) for a, b in zip(edges, edges[1:])]


def merge_gather(n, wq, wk, wv, lq, lk, lv, hq, hk, hv, fq, fk, fv, cq, ck, cv,
                 rq, rk, rv, maxes, max_send, max_recv, send_sem, recv_sem):
    me = lax.axis_index("fsdp")
    half = n // 2

    def at(p):
        p = lax.rem(p + 2 * n, n)
        side = p // half
        z = p + side * (n - 1 - 2 * p)
        return z * 2 + side

    z, x = me // 2, lax.rem(me, 2)
    pos = z + x * (n - 1 - 2 * z)

    barrier = pltpu.get_barrier_semaphore()
    for d in range(1, n):
        pl.semaphore_signal(barrier, inc=1, device_id={"fsdp": lax.rem(me + d, n)}, device_id_type=MESH)

    rows = wq.shape[0]
    step_rows = 64 if rows % 64 == 0 else rows
    groups = ((wq, lq, hq, rq, cq, fq), (wk, lk, hk, rk, ck, fk), (wv, lv, hv, rv, cv, fv))
    start = 0
    spans = []
    for w, low, high, res, _, _ in groups:
        width = w.shape[1]
        tile = min(width, 512)
        for c in range(0, width, tile):
            cols = slice(c, c + tile)
            delta = lax.dot_general(low[...], high[:, cols], (((0,), (0,)), ((), ())),
                                    preferred_element_type=jnp.float32)
            out = w[:, cols].astype(jnp.float32) + mix_rate * delta
            res[:, cols] = out
            maxes[me, :, start + c:start + c + tile] = jnp.max(jnp.abs(out), axis=0, keepdims=True)
        spans.append((start, width))
        start += width

    pl.semaphore_wait(barrier, n - 1)
    copies = []
    for d in range(1, n):
        copy = pltpu.make_async_remote_copy(
            src_ref=maxes.at[me], dst_ref=maxes.at[me],
            send_sem=max_send.at[d], recv_sem=max_recv.at[d],
            device_id={"fsdp": lax.rem(me + d, n)}, device_id_type=MESH)
        copy.start()
        copies.append(copy)
    for copy in copies:
        copy.wait()

    base = pl.multiple_of(me * rows, rows)
    for (s, width), (_, _, _, res, col, fin) in zip(spans, groups):
        top = jnp.max(maxes[:, 0, s:s + width], axis=0, keepdims=True)
        col[...] = top

        @pl.loop(0, rows // step_rows)
        def _(i):
            r = pl.multiple_of(i * step_rows, step_rows)
            fin[pl.ds(base + r, step_rows), :] = (res[pl.ds(r, step_rows), :] / top).astype(jnp.bfloat16)

    h = rows // 2
    pieces = [(fq, a, b) for a, b in split_rows(h, QUERY_PIECES)] + [(fk, 0, h), (fv, 0, h)]
    count = len(pieces)

    def piece_copy(step, which, k):
        ref, a, size = pieces[k]
        sign = 1 - 2 * which
        owner = at(pos - sign * step)
        window = ref.at[pl.ds(pl.multiple_of(owner * rows + which * h + a, 16), size)]
        i = (step * 2 + which) * count + k
        return pltpu.make_async_remote_copy(
            src_ref=window, dst_ref=window, send_sem=send_sem.at[i], recv_sem=recv_sem.at[i],
            device_id={"fsdp": at(pos + sign)}, device_id_type=MESH)

    def arrival(step, which, k):
        ref, a, size = pieces[k]
        sign = 1 - 2 * which
        owner = at(pos - sign * (step + 1))
        window = ref.at[pl.ds(pl.multiple_of(owner * rows + which * h + a, 16), size)]
        i = (step * 2 + which) * count + k
        pltpu.make_async_remote_copy(
            src_ref=window, dst_ref=window, send_sem=send_sem.at[i], recv_sem=recv_sem.at[i],
            device_id={"fsdp": at(pos + sign)}, device_id_type=MESH).wait_recv()

    for k in range(count):
        for which in range(2):
            piece_copy(0, which, k).start()

    @pl.loop(1, n - 1)
    def _(step):
        for k in range(count):
            for which in range(2):
                arrival(step - 1, which, k)
                piece_copy(step, which, k).start()

    for k in range(count):
        for which in range(2):
            arrival(n - 2, which, k)

    @pl.loop(0, n - 1)
    def _(step):
        for k in range(count):
            for which in range(2):
                piece_copy(step, which, k).wait_send()


def solution(mesh):
    n = mesh.shape["fsdp"]

    def per_device(wq, lq, hq, wk, lk, hk, wv, lv, hv, norm_train, norm_step):
        rows = wq.shape[0]
        widths = [w.shape[1] for w in (wq, wk, wv)]
        count = len(split_rows(rows // 2, QUERY_PIECES)) + 2
        vmem = pl.BlockSpec(memory_space=pltpu.VMEM)
        fq, fk, fv, cq, ck, cv = pl.pallas_call(
            functools.partial(merge_gather, n),
            out_shape=[pltpu.VMEM((n * rows, w), jnp.bfloat16) for w in widths]
            + [jax.ShapeDtypeStruct((1, w), jnp.float32) for w in widths],
            in_specs=[vmem] * 9,
            out_specs=[vmem] * 6,
            scratch_shapes=[pltpu.VMEM((rows, w), jnp.float32) for w in widths]
            + [
                pltpu.VMEM((n, 1, sum(widths)), jnp.float32),
                pltpu.SemaphoreType.DMA((n,)),
                pltpu.SemaphoreType.DMA((n,)),
                pltpu.SemaphoreType.DMA(((n - 1) * 2 * count,)),
                pltpu.SemaphoreType.DMA(((n - 1) * 2 * count,)),
            ],
            compiler_params=pltpu.CompilerParams(
                collective_id=0, has_side_effects=True, vmem_limit_bytes=24 * 1024 * 1024),
        )(wq, wk, wv, lq.T, lk.T, lv.T, hq, hk, hv)
        serve_norm = lax.all_gather(
            (norm_train + norm_step).astype(jnp.bfloat16), ("fsdp", "model"), axis=0, tiled=True)
        return (fq, fk, fv, cq.reshape(-1), ck.reshape(-1), cv.reshape(-1), serve_norm)

    return jax.shard_map(
        per_device,
        mesh=mesh,
        in_specs=(
            P("fsdp", "model"), P("fsdp", None), P(None, "model"),
            P("fsdp", "model"), P("fsdp", None), P(None, "model"),
            P("fsdp", "model"), P("fsdp", None), P(None, "model"),
            P(("fsdp", "model")), P(("fsdp", "model")),
        ),
        out_specs=(P(None, "model"), P(None, "model"), P(None, "model"),
                   P("model"), P("model"), P("model"), P()),
        check_vma=False,
    )
```

```python
import functools

import jax
import jax.numpy as jnp
from jax import lax
from jax.experimental import pallas as pl
from jax.experimental.pallas import tpu as pltpu
from jax.sharding import PartitionSpec as P

mix_rate = 0.5
MESH = pl.DeviceIdType.MESH
QUERY_PIECES = 4


def split_rows(rows, parts):
    tiles = rows // 16
    parts = min(parts, tiles)
    edges = [16 * (tiles * i // parts) for i in range(parts + 1)]
    return [(a, b - a) for a, b in zip(edges, edges[1:])]


def merge_gather(n, m, hwq, hwk, hwv, hlq, hlk, hlv, hhq, hhk, hhv, htrain, hstep,
                 fq, fk, fv, cq, ck, cv, gains,
                 wq, wk, wv, lq, lk, lv, hq, hk, hv, train, step_gain, own_gain,
                 rq, rk, rv, maxes, load_sem, max_send, max_recv, gain_send, gain_recv, send_sem, recv_sem):
    me = lax.axis_index("fsdp")
    lane = lax.axis_index("model")
    half = n // 2

    def at(p):
        p = lax.rem(p + 2 * n, n)
        side = p // half
        z = p + side * (n - 1 - 2 * p)
        return z * 2 + side

    z, x = me // 2, lax.rem(me, 2)
    pos = z + x * (n - 1 - 2 * z)

    staged = ((hwk, wk), (hlk, lk), (hhk, hk), (hwv, wv), (hlv, lv), (hhv, hv),
              (hwq, wq), (hlq, lq), (hhq, hq), (htrain, train), (hstep, step_gain))
    loads = [pltpu.make_async_copy(src, dst, load_sem.at[i]) for i, (src, dst) in enumerate(staged)]
    for load in loads:
        load.start()

    barrier = pltpu.get_barrier_semaphore()
    others = [(d, e) for d in range(n) for e in range(m) if d or e]

    def peer(d, e):
        return {"fsdp": lax.rem(me + d, n), "model": lax.rem(lane + e, m)}

    for d, e in others:
        pl.semaphore_signal(barrier, inc=1, device_id=peer(d, e), device_id_type=MESH)

    rows = wq.shape[0]
    step_rows = 64 if rows % 64 == 0 else rows
    groups = ((wk, lk, hk, rk, ck, fk), (wv, lv, hv, rv, cv, fv), (wq, lq, hq, rq, cq, fq))
    start = 0
    spans = []
    for g, (w, low, high, res, _, _) in enumerate(groups):
        for load in loads[3 * g:3 * g + 3]:
            load.wait()
        width = w.shape[1]
        tile = min(width, 512)
        for c in range(0, width, tile):
            cols = slice(c, c + tile)
            delta = lax.dot_general(low[...], high[:, cols], (((0,), (0,)), ((), ())),
                                    preferred_element_type=jnp.float32)
            out = w[:, cols].astype(jnp.float32) + mix_rate * delta
            res[:, cols] = out
            maxes[me, :, start + c:start + c + tile] = jnp.max(jnp.abs(out), axis=0, keepdims=True)
        spans.append((start, width))
        start += width
    for load in loads[9:]:
        load.wait()
    own_gain[...] = train[...] + step_gain[...]

    pl.semaphore_wait(barrier, len(others))
    copies = []
    for d in range(1, n):
        copy = pltpu.make_async_remote_copy(
            src_ref=maxes.at[me], dst_ref=maxes.at[me],
            send_sem=max_send.at[d], recv_sem=max_recv.at[d],
            device_id=peer(d, 0), device_id_type=MESH)
        copy.start()
        copies.append(copy)
    for copy in copies:
        copy.wait()

    base = pl.multiple_of(me * rows, rows)
    for (s, width), (_, _, _, res, col, fin) in zip(spans, groups):
        top = jnp.max(maxes[:, 0, s:s + width], axis=0, keepdims=True)
        col[...] = top

        @pl.loop(0, rows // step_rows)
        def _(i):
            r = pl.multiple_of(i * step_rows, step_rows)
            fin[pl.ds(base + r, step_rows), :] = (res[pl.ds(r, step_rows), :] / top).astype(jnp.bfloat16)

    h = rows // 2
    pieces = [(fq, a, b) for a, b in split_rows(h, QUERY_PIECES)] + [(fk, 0, h), (fv, 0, h)]
    count = len(pieces)

    def piece_copy(step, which, k):
        ref, a, size = pieces[k]
        sign = 1 - 2 * which
        owner = at(pos - sign * step)
        window = ref.at[pl.ds(pl.multiple_of(owner * rows + which * h + a, 16), size)]
        i = (step * 2 + which) * count + k
        return pltpu.make_async_remote_copy(
            src_ref=window, dst_ref=window, send_sem=send_sem.at[i], recv_sem=recv_sem.at[i],
            device_id={"fsdp": at(pos + sign)}, device_id_type=MESH)

    def arrival(step, which, k):
        ref, a, size = pieces[k]
        sign = 1 - 2 * which
        owner = at(pos - sign * (step + 1))
        window = ref.at[pl.ds(pl.multiple_of(owner * rows + which * h + a, 16), size)]
        i = (step * 2 + which) * count + k
        pltpu.make_async_remote_copy(
            src_ref=window, dst_ref=window, send_sem=send_sem.at[i], recv_sem=recv_sem.at[i],
            device_id={"fsdp": at(pos + sign)}, device_id_type=MESH).wait_recv()

    for k in range(count):
        for which in range(2):
            piece_copy(0, which, k).start()

    gain_copies = []
    for i, (d, e) in enumerate(others):
        copy = pltpu.make_async_remote_copy(
            src_ref=own_gain, dst_ref=gains.at[me * m + lane],
            send_sem=gain_send.at[i], recv_sem=gain_recv.at[i],
            device_id=peer(d, e), device_id_type=MESH)
        copy.start()
        gain_copies.append(copy)
    gains[me * m + lane] = own_gain[...]
    for copy in gain_copies:
        copy.wait()

    @pl.loop(1, n - 1)
    def _(step):
        for k in range(count):
            for which in range(2):
                arrival(step - 1, which, k)
                piece_copy(step, which, k).start()

    for k in range(count):
        for which in range(2):
            arrival(n - 2, which, k)

    @pl.loop(0, n - 1)
    def _(step):
        for k in range(count):
            for which in range(2):
                piece_copy(step, which, k).wait_send()


def write_out(sizes, *refs):
    count = len(sizes)
    srcs, dsts, sem = refs[:count], refs[count:2 * count], refs[2 * count]
    copies = []
    for src, dst, parts in zip(srcs, dsts, sizes):
        size = src.shape[0] // parts
        for p in range(parts):
            window = pl.ds(p * size, size)
            copies.append(pltpu.make_async_copy(src.at[window], dst.at[window], sem.at[len(copies)]))
    for copy in copies:
        copy.start()
    for copy in copies:
        copy.wait()


def solution(mesh):
    n, m = mesh.shape["fsdp"], mesh.shape["model"]

    def per_device(wq, lq, hq, wk, lk, hk, wv, lv, hv, norm_train, norm_step):
        rows = wq.shape[0]
        widths = [w.shape[1] for w in (wq, wk, wv)]
        count = len(split_rows(rows // 2, QUERY_PIECES)) + 2
        own = norm_train.shape[0]
        hbm = pl.BlockSpec(memory_space=pltpu.HBM)
        vmem = pl.BlockSpec(memory_space=pltpu.VMEM)
        args = (wq, wk, wv, lq.T, lk.T, lv.T, hq, hk, hv, norm_train.reshape(1, own), norm_step.reshape(1, own))
        *held, gains = pl.pallas_call(
            functools.partial(merge_gather, n, m),
            out_shape=[pltpu.VMEM((n * rows, w), jnp.bfloat16) for w in widths]
            + [pltpu.VMEM((1, w), jnp.float32) for w in widths]
            + [pltpu.VMEM((n * m, 1, own), jnp.float32)],
            in_specs=[hbm] * len(args),
            out_specs=[vmem] * 7,
            scratch_shapes=[pltpu.VMEM(a.shape, a.dtype) for a in args]
            + [pltpu.VMEM((1, own), jnp.float32)]
            + [pltpu.VMEM((rows, w), jnp.float32) for w in widths]
            + [
                pltpu.VMEM((n, 1, sum(widths)), jnp.float32),
                pltpu.SemaphoreType.DMA((len(args),)),
                pltpu.SemaphoreType.DMA((n,)),
                pltpu.SemaphoreType.DMA((n,)),
                pltpu.SemaphoreType.DMA((n * m,)),
                pltpu.SemaphoreType.DMA((n * m,)),
                pltpu.SemaphoreType.DMA(((n - 1) * 2 * count,)),
                pltpu.SemaphoreType.DMA(((n - 1) * 2 * count,)),
            ],
            compiler_params=pltpu.CompilerParams(
                collective_id=0, has_side_effects=True, vmem_limit_bytes=67043328 - 2 * n * rows * sum(widths) - 4 * 8 * sum(widths) - 32768 * 4 - 1048576),
        )(*args)
        sizes = (8, 2, 2, 1, 1, 1)
        fq, fk, fv, cq, ck, cv = pl.pallas_call(
            functools.partial(write_out, sizes),
            out_shape=[jax.ShapeDtypeStruct(a.shape, a.dtype) for a in held],
            in_specs=[vmem] * 6,
            out_specs=[hbm] * 6,
            scratch_shapes=[pltpu.SemaphoreType.DMA((sum(sizes),))],
            compiler_params=pltpu.CompilerParams(vmem_limit_bytes=1024 * 1024),
        )(*held)
        serve_norm = gains.reshape(-1).astype(jnp.bfloat16)
        return (fq, fk, fv, cq.reshape(-1), ck.reshape(-1), cv.reshape(-1), serve_norm)

    return jax.shard_map(
        per_device,
        mesh=mesh,
        in_specs=(
            P("fsdp", "model"), P("fsdp", None), P(None, "model"),
            P("fsdp", "model"), P("fsdp", None), P(None, "model"),
            P("fsdp", "model"), P("fsdp", None), P(None, "model"),
            P(("fsdp", "model")), P(("fsdp", "model")),
        ),
        out_specs=(P(None, "model"), P(None, "model"), P(None, "model"),
                   P("model"), P("model"), P("model"), P()),
        check_vma=False,
    )
```
